32 devices in a mesh: track: 4 (over y, x), ifg: 4 (over z), pix: 2 (over core).
Axes of the slice: x: 2, y: 2, z: 4, core: 2. Of those that a mesh axis runs over, the one named last changes fastest.
Arguments:
- phases: bfloat16 [4, 600, 32768], P('track', 'ifg', 'pix')
- pairs: int32 [4, 600, 2], P('track', 'ifg'), may hold values from 0 to 249, as said below
- date_map: int32 [4, 250], replicated, may hold values from 0 to 319, as said below
- knots: int32 [32], replicated, may hold values from 0 to 319, as said below
- look: float32 [4, 3, 32768], P(None, None, 'pix'), may hold values from -1 to 1
Outputs:
- enu: float32 [3, 320, 32768], P(None, None, ('pix', 'ifg', 'track'))
- spline: float32 [3, 32, 32768], P(None, None, ('pix', 'ifg', 'track'))
The draws below stay inside these ranges and needn't reach their ends.
Inputs may be any that keep to these rules, and one draw needn't show every extreme that they name: pairs[t, k, 0] < pairs[t, k, 1] <= pairs[t, k, 0] + 5. `date_map`: the dates of one track map to distinct epochs. `knots`: strictly increasing, the first 0 and the last 319.
All inputs are finite; a program needn't handle non-finite values.
Results may differ from the reference program's by a relative error of at most 0.0003.
Values may be sent and summed in bfloat16 or wider, within the bound.
A program may use at most 128 MiB of HBM per device.

```python
import jax
import jax.numpy as jnp
from jax import lax

NDATE = 250
IFGS = 600
EPOCHS = 320
KNOTS = 32
SPAN = 5
PIX_DEV = 16384
TRACKS = 4
PIXELS = 32768
N_TRACK = 4
N_IFG = 4


def draw_phases(key, part):
    key_common, key_noise = jax.random.split(key, 2)
    common = 2.0 * jax.random.normal(key_common, (TRACKS, IFGS, 1), jnp.float32)
    ramp = 1.0 + 2.0 * jnp.arange(PIXELS, dtype=jnp.float32)[None, None, :] / PIXELS
    noise = jax.random.normal(key_noise, (TRACKS, IFGS, PIXELS), jnp.float32)
    values = common * ramp + noise
    return values.astype(jnp.bfloat16)


def draw_pairs(key, part):
    key_first, key_step = jax.random.split(key)
    first = jax.random.randint(key_first, (TRACKS, IFGS), 0, NDATE - SPAN)
    step = jax.random.randint(key_step, (TRACKS, IFGS), 1, SPAN + 1)
    first = first.at[:, 0].set(0).at[:, IFGS - 1].set(NDATE - 1 - SPAN)
    step = step.at[:, IFGS - 1].set(SPAN)
    return jnp.stack([first, first + step], axis=-1).astype(jnp.int32)


def draw_date_map(key, part):
    scores = jax.random.randint(key, (TRACKS, EPOCHS), 0, 2 ** 20) * EPOCHS + jnp.arange(EPOCHS, dtype=jnp.int32)[None, :]
    index = jnp.arange(EPOCHS, dtype=jnp.int32)[None, :]
    scores = jnp.where((index == 0) | (index == EPOCHS - 1), 2 ** 30, scores)
    chosen = lax_top(scores, NDATE)
    return jnp.sort(chosen, axis=1).astype(jnp.int32)


def lax_top(scores, count):
    return jax.lax.top_k(scores, count)[1].astype(jnp.int32)


def draw_knots(key, part):
    scores = jax.random.randint(key, (EPOCHS - 2,), 0, 2 ** 20) * EPOCHS + jnp.arange(EPOCHS - 2, dtype=jnp.int32)
    inner = jnp.sort(lax_top(scores, KNOTS - 2)) + 1
    head = jnp.zeros((1,), jnp.int32)
    tail = jnp.full((1,), EPOCHS - 1, jnp.int32)
    return jnp.concatenate([head, inner.astype(jnp.int32), tail]).astype(jnp.int32)


def shard_levels(rng, dims, pieces, least, top_value):
    level, own = 1.0, jax.random.fold_in(rng, 6)
    for axis_at, shards_of in pieces:
        steps = jnp.exp(jax.random.uniform(jax.random.fold_in(own, axis_at), (shards_of,), jnp.float32, least / len(pieces), top_value / len(pieces)))
        level = level * jnp.repeat(steps, dims[axis_at] // shards_of).reshape([-1 if axis == axis_at else 1 for axis in range(len(dims))])
    return level


def setup_inputs(seed: int = 0) -> dict:
    arg_keys = jax.random.split(jax.random.key(seed), 6)
    return {
        "phases": draw_phases(jax.random.fold_in(arg_keys[5], 71), 0),
        "pairs": draw_pairs(jax.random.fold_in(arg_keys[5], 71), 0),
        "date_map": draw_date_map(jax.random.fold_in(arg_keys[5], 71), 0),
        "knots": draw_knots(jax.random.fold_in(arg_keys[5], 71), 0),
        "look": jnp.clip(jax.random.uniform(arg_keys[4], (TRACKS, 3, PIXELS), jnp.float32, -1.0, 1.0) * shard_levels(arg_keys[4], (TRACKS, 3, PIXELS), ((2, 2),), -0.4, 0.0), -1.0, 1.0),
    }


damping = 0.5
ridge = 0.1
HIGH = lax.Precision.HIGHEST

def incidence(pair_rows, ndate):
    dates = jnp.arange(ndate, dtype=jnp.int32)[:, None]
    later = (dates == pair_rows[None, :, 1]).astype(jnp.float32)
    earlier = (dates == pair_rows[None, :, 0]).astype(jnp.float32)
    return later - earlier

def inverse_normal(incid):
    ndate = incid.shape[0]
    normal = jnp.dot(incid, incid.T, precision=HIGH) + damping * jnp.eye(ndate, dtype=jnp.float32)
    factor = jnp.linalg.cholesky(normal)
    return jax.scipy.linalg.cho_solve((factor, True), jnp.eye(ndate, dtype=jnp.float32))

def hat_basis(knots, n_epochs):
    spots = knots.astype(jnp.float32)
    left = jnp.concatenate([spots[:1] - 1.0, spots[:-1]])
    right = jnp.concatenate([spots[1:], spots[-1:] + 1.0])
    epochs = jnp.arange(n_epochs, dtype=jnp.float32)[:, None]
    rise = (epochs - left) / (spots - left)
    fall = (right - epochs) / (right - spots)
    return jnp.maximum(0.0, jnp.minimum(rise, fall))

def geometry(series, date_map, look, knots, n_epochs):
    epochs = jnp.arange(n_epochs, dtype=jnp.int32)
    onehot = (date_map[:, None, :] == epochs[None, :, None]).astype(jnp.float32)
    seen = jnp.sum(onehot, axis=2)
    resampled = jnp.einsum('tcd,tdp->tcp', onehot, series, precision=HIGH)

    def entry(first, second):
        value = jnp.einsum('tc,tp->cp', seen, look[:, first] * look[:, second], precision=HIGH)
        if first == second:
            value = value + ridge
        return value
    a00, a01, a02 = (entry(0, 0), entry(0, 1), entry(0, 2))
    a11, a12, a22 = (entry(1, 1), entry(1, 2), entry(2, 2))
    b_all = [jnp.sum(look[:, i][:, None, :] * resampled, axis=0) for i in range(3)]
    c00 = a11 * a22 - a12 * a12
    c01 = a02 * a12 - a01 * a22
    c02 = a01 * a12 - a02 * a11
    c11 = a00 * a22 - a02 * a02
    c12 = a01 * a02 - a00 * a12
    c22 = a00 * a11 - a01 * a01
    det = a00 * c00 + a01 * c01 + a02 * c02
    east = (c00 * b_all[0] + c01 * b_all[1] + c02 * b_all[2]) / det
    north = (c01 * b_all[0] + c11 * b_all[1] + c12 * b_all[2]) / det
    upward = (c02 * b_all[0] + c12 * b_all[1] + c22 * b_all[2]) / det
    enu = jnp.stack([east, north, upward])
    basis = hat_basis(knots, n_epochs)
    gram = jnp.dot(basis.T, basis, precision=HIGH)
    factor = jnp.linalg.cholesky(gram)
    fitter = jax.scipy.linalg.cho_solve((factor, True), basis.T)
    spline = jnp.einsum('kc,icp->ikp', fitter, enu, precision=HIGH)
    return (enu, spline)

def reference(phases, pairs, date_map, knots, look):
    stacked = []
    for track in range(TRACKS):
        incid = incidence(pairs[track], NDATE)
        ninv = inverse_normal(incid)
        rhs = jnp.dot(incid.astype(jnp.bfloat16).astype(jnp.float32), phases[track].astype(jnp.float32), preferred_element_type=jnp.float32)
        series = jnp.dot(ninv, rhs, precision=HIGH)
        series = series - jnp.mean(series, axis=1, keepdims=True)
        stacked.append(series)
    series_all = jnp.stack(stacked)
    width = PIX_DEV // (N_IFG * N_TRACK)
    blocks = PIXELS // width
    series_blocks = jnp.transpose(series_all.reshape(TRACKS, NDATE, blocks, width), (2, 0, 1, 3))
    look_blocks = jnp.transpose(look.reshape(TRACKS, 3, blocks, width), (2, 0, 1, 3))

    def one_block(items):
        return geometry(items[0], date_map, items[1], knots, EPOCHS)
    enu_blocks, spline_blocks = lax.map(one_block, (series_blocks, look_blocks))
    enu = jnp.transpose(enu_blocks, (1, 2, 0, 3)).reshape(3, EPOCHS, PIXELS)
    spline = jnp.transpose(spline_blocks, (1, 2, 0, 3)).reshape(3, KNOTS, PIXELS)
    return (enu, spline)
```

```python
import functools
import math

import jax
import jax.numpy as jnp
from jax import lax
from jax.experimental import pallas as pl
from jax.experimental.pallas import tpu as pltpu
from jax.sharding import PartitionSpec as P

EPOCHS = 320
DAMPING = 0.5
RIDGE = 0.1
HIGH = lax.Precision.HIGHEST
MESH = pl.DeviceIdType.MESH
NT = (((1,), (1,)), ((), ()))


def dot(a, b):
    return jnp.dot(a, b, precision=HIGH, preferred_element_type=jnp.float32)


def partner(index, step, count):
    if count & (count - 1) == 0:
        return lax.bitwise_xor(index, step)
    return lax.rem(index + step, count)


def exchange_kernel(n_track, n_ifg, n_pix, pixels, ndate, ph, pairs, dmap, spots, out, r_out, meta, fitter,
                    pairs_all, normal, inverse, r_full, local, sums_pix, sums_all,
                    send, recv, p_send, p_recv, x_send, x_recv, s_send, s_recv, l_sem):
    t, i, x = lax.axis_index("track"), lax.axis_index("ifg"), lax.axis_index("pix")
    width = out.shape[-1]
    ifgs = ph.shape[0]
    epochs = fitter.shape[1]
    order = sorted(range(n_ifg), key=lambda s: (s == 0, -(s >= n_ifg // 2), s))
    steps = [(dt, di) for di in order for dt in reversed(range(n_track)) if (dt, di) != (0, 0)]

    def peer(dt, di):
        return {"track": partner(t, dt, n_track), "ifg": partner(i, di, n_ifg)}

    bar = pltpu.get_barrier_semaphore()
    for dt, di in steps:
        pl.semaphore_signal(bar, inc=1, device_id=peer(dt, di), device_id_type=MESH)
    for dx in range(1, n_pix):
        pl.semaphore_signal(bar, inc=1, device_id={"pix": partner(x, dx, n_pix)}, device_id_type=MESH)
    pl.semaphore_wait(bar, len(steps) + n_pix - 1)

    def remote(src, dst, ssem, rsem, device):
        return pltpu.make_async_remote_copy(src_ref=src, dst_ref=dst, send_sem=ssem, recv_sem=rsem,
                                            device_id=device, device_id_type=MESH)

    pair_copies, phase_copies = [], []
    for dt, di in steps:
        at = dt * n_ifg + di
        copy = remote(pairs, pairs_all.at[t, i], p_send.at[at], p_recv.at[at], peer(dt, di))
        copy.start()
        pair_copies.append(copy)

    def send_phases(dt, di):
        at = dt * n_ifg + di
        where = peer(dt, di)
        column = pl.multiple_of((where["ifg"] * n_track + where["track"]) * width, width)
        copy = remote(ph.at[:, pl.ds(column, width)], out.at[t, i], send.at[at], recv.at[at], where)
        copy.start()
        phase_copies.append(copy)

    early = [s for s in steps if s[1] >= max(1, n_ifg // 2)]
    late = [s for s in steps if s not in early]
    for s in early:
        send_phases(*s)
    load = pltpu.make_async_copy(ph, local, l_sem.at[0])
    load.start()
    own_pairs = pltpu.make_async_copy(pairs, pairs_all.at[t, i], l_sem.at[1])
    own_pairs.start()
    column = pl.multiple_of((i * n_track + t) * width, width)
    own = pltpu.make_async_copy(ph.at[:, pl.ds(column, width)], out.at[t, i], l_sem.at[2])
    own.start()

    load.wait()
    ones = jnp.ones((8, width), jnp.bfloat16)

    def add_columns(step, total):
        part = local[:, pl.ds(pl.multiple_of(step * width, width), width)]
        return total + lax.dot_general(ones, part, NT, preferred_element_type=jnp.float32)

    row_sums = lax.fori_loop(0, ph.shape[1] // width, add_columns, jnp.zeros((8, ifgs), jnp.float32))
    sums_pix[x] = row_sums

    own_pairs.wait()
    for copy in pair_copies:
        copy.wait()

    def incidence(track, piece):
        dates = lax.broadcasted_iota(jnp.int32, (ndate, ifgs), 0)
        first = pairs_all[track, piece, 0:1, :]
        second = pairs_all[track, piece, 1:2, :]
        return (dates == second).astype(jnp.float32) - (dates == first).astype(jnp.float32)

    def eye(n):
        return (lax.broadcasted_iota(jnp.int32, (n, n), 0) == lax.broadcasted_iota(jnp.int32, (n, n), 1)).astype(jnp.float32)

    total_ifgs = ifgs * n_ifg
    scale = 2.0 / (2.0 * DAMPING + 2.0 * total_ifgs)
    for track in range(n_track):
        value = DAMPING * eye(ndate)
        for piece in range(n_ifg):
            part = incidence(track, piece).astype(jnp.bfloat16)
            value = value + lax.dot_general(part, part, NT, preferred_element_type=jnp.float32)
        normal[track] = value
        inverse[track] = scale * eye(ndate)

    pix_copies = []
    for dx in range(1, n_pix):
        copy = remote(sums_pix.at[x], sums_pix.at[x], x_send.at[dx], x_recv.at[dx], {"pix": partner(x, dx, n_pix)})
        copy.start()
        pix_copies.append(copy)
    for copy in pix_copies:
        copy.wait()
    gathered = sums_pix[0]
    for k in range(1, n_pix):
        gathered = gathered + sums_pix[k]
    sums_all[t, i] = gathered

    spot, left, right = spots[0:1, :], spots[1:2, :], spots[2:3, :]
    knots = spots.shape[1]
    epoch = lax.broadcasted_iota(jnp.int32, (epochs, knots), 0).astype(jnp.float32)
    basis = jnp.maximum(0.0, jnp.minimum((epoch - left) / (spot - left), (right - epoch) / (right - spot)))
    gram = lax.dot_general(basis, basis, (((0,), (0,)), ((), ())), precision=HIGH, preferred_element_type=jnp.float32)
    unit = eye(knots)
    guess = unit / jnp.sum(gram * unit, axis=1, keepdims=True)
    for _ in range(6):
        guess = 2.0 * guess - dot(guess, dot(gram, guess))
    fitter[...] = lax.dot_general(guess, basis, NT, precision=HIGH, preferred_element_type=jnp.float32)

    sum_copies = []
    for dt, di in steps:
        at = dt * n_ifg + di
        copy = remote(sums_all.at[t, i], sums_all.at[t, i], s_send.at[at], s_recv.at[at], peer(dt, di))
        copy.start()
        sum_copies.append(copy)
    for s in late:
        send_phases(*s)

    rounds = math.ceil(math.log2(18.0 * (1.0 + 2.0 * total_ifgs / (2.0 * DAMPING)))) + 1

    def newton(_, carry):
        for track in range(n_track):
            now = inverse[track]
            inverse[track] = 2.0 * now - dot(now, dot(normal[track], now))
        return carry

    lax.fori_loop(0, rounds, newton, 0)

    for track in range(n_track):
        hot = (lax.broadcasted_iota(jnp.int32, (epochs, ndate), 0) == dmap[track:track + 1, :]).astype(jnp.float32)
        rows = dot(hot, inverse[track])
        for piece in range(n_ifg):
            full = dot(rows, incidence(track, piece))
            r_full[track, piece] = full
            high = full.astype(jnp.bfloat16)
            r_out[track, piece, :epochs, :] = high
            r_out[track, piece, epochs:, :] = (full - high.astype(jnp.float32)).astype(jnp.bfloat16)

    for copy in sum_copies:
        copy.wait()
    for track in range(n_track):
        hot = (lax.broadcasted_iota(jnp.int32, (epochs, ndate), 0) == dmap[track:track + 1, :]).astype(jnp.float32)
        seen = jnp.sum(hot, axis=1, keepdims=True)
        mean = jnp.zeros((epochs, 1), jnp.float32)
        for piece in range(n_ifg):
            mean = mean + jnp.sum(r_full[track, piece] * sums_all[track, piece, 0:1, :], axis=1, keepdims=True)
        lane = lax.broadcasted_iota(jnp.int32, (epochs, 128), 1)
        meta[track] = jnp.where(lane == 0, mean * (1.0 / pixels), seen)
    own.wait()
    for copy in phase_copies:
        copy.wait()


def geometry_kernel(ph, r, meta, fitter, look, enu, spline):
    n_track, n_ifg = ph.shape[:2]
    epochs = enu.shape[1]
    terms = []
    for track in range(n_track):
        both = jnp.dot(r[track, 0], ph[track, 0], preferred_element_type=jnp.float32)
        for piece in range(1, n_ifg):
            both = both + jnp.dot(r[track, piece], ph[track, piece], preferred_element_type=jnp.float32)
        terms.append(both[:epochs] + both[epochs:] - meta[track, :, 0:1])
    seen = [meta[track, :, 1:2] for track in range(n_track)]
    rows = [[look[track, j:j + 1, :] for j in range(3)] for track in range(n_track)]

    def entry(a, b):
        value = RIDGE if a == b else 0.0
        for track in range(n_track):
            value = value + seen[track] * (rows[track][a] * rows[track][b])
        return value

    a00, a01, a02 = entry(0, 0), entry(0, 1), entry(0, 2)
    a11, a12, a22 = entry(1, 1), entry(1, 2), entry(2, 2)
    b = []
    for j in range(3):
        value = rows[0][j] * terms[0]
        for track in range(1, n_track):
            value = value + rows[track][j] * terms[track]
        b.append(value)
    c00 = a11 * a22 - a12 * a12
    c01 = a02 * a12 - a01 * a22
    c02 = a01 * a12 - a02 * a11
    c11 = a00 * a22 - a02 * a02
    c12 = a01 * a02 - a00 * a12
    c22 = a00 * a11 - a01 * a01
    inv = 1.0 / (a00 * c00 + a01 * c01 + a02 * c02)
    enu[0] = (c00 * b[0] + c01 * b[1] + c02 * b[2]) * inv
    enu[1] = (c01 * b[0] + c11 * b[1] + c12 * b[2]) * inv
    enu[2] = (c02 * b[0] + c12 * b[1] + c22 * b[2]) * inv
    for j in range(3):
        spline[j] = dot(fitter[...], enu[j])


def shards(sizes, phases, pairs, date_map, knots, look):
    n_track, n_ifg, n_pix = sizes
    ifgs, columns = phases.shape[1:]
    width = columns // (n_track * n_ifg)
    ndate, n_knots = date_map.shape[1], knots.shape[0]
    peers = n_track * n_ifg
    spots = knots.astype(jnp.float32)
    spots = jnp.stack([spots, jnp.concatenate([spots[:1] - 1.0, spots[:-1]]),
                       jnp.concatenate([spots[1:], spots[-1:] + 1.0])])
    vmem = pl.BlockSpec(memory_space=pltpu.VMEM)
    anywhere = pl.BlockSpec(memory_space=pl.ANY)
    dma = lambda n: pltpu.SemaphoreType.DMA((n,))
    gathered, r, meta, fitter = pl.pallas_call(
        functools.partial(exchange_kernel, n_track, n_ifg, n_pix, columns * n_pix, ndate),
        out_shape=(
            jax.ShapeDtypeStruct((n_track, n_ifg, ifgs, width), phases.dtype),
            jax.ShapeDtypeStruct((n_track, n_ifg, 2 * EPOCHS, ifgs), jnp.bfloat16),
            jax.ShapeDtypeStruct((n_track, EPOCHS, 128), jnp.float32),
            jax.ShapeDtypeStruct((n_knots, EPOCHS), jnp.float32),
        ),
        in_specs=[anywhere, vmem, vmem, vmem],
        out_specs=(anywhere, vmem, vmem, vmem),
        scratch_shapes=[
            pltpu.VMEM((n_track, n_ifg, 2, ifgs), jnp.int32),
            pltpu.VMEM((n_track, ndate, ndate), jnp.float32),
            pltpu.VMEM((n_track, ndate, ndate), jnp.float32),
            pltpu.VMEM((n_track, n_ifg, EPOCHS, ifgs), jnp.float32),
            pltpu.VMEM((ifgs, columns), phases.dtype),
            pltpu.VMEM((n_pix, 8, ifgs), jnp.float32),
            pltpu.VMEM((n_track, n_ifg, 8, ifgs), jnp.float32),
            dma(peers), dma(peers), dma(peers), dma(peers), dma(n_pix), dma(n_pix), dma(peers), dma(peers), dma(3),
        ],
        compiler_params=pltpu.CompilerParams(collective_id=0, has_side_effects=True, vmem_limit_bytes=48 << 20),
        name="exchange",
    )(phases[0], pairs[0].T, date_map, spots)

    offset = (lax.axis_index("ifg") * n_track + lax.axis_index("track")) * width
    look_local = lax.dynamic_slice_in_dim(look, offset, width, 2)
    block = min(256, width)
    return tuple(pl.pallas_call(
        geometry_kernel,
        grid=(width // block,),
        out_shape=(
            jax.ShapeDtypeStruct((3, EPOCHS, width), jnp.float32),
            jax.ShapeDtypeStruct((3, n_knots, width), jnp.float32),
        ),
        in_specs=[
            pl.BlockSpec((n_track, n_ifg, ifgs, block), lambda g: (0, 0, 0, g)),
            pl.BlockSpec((n_track, n_ifg, 2 * EPOCHS, ifgs), lambda g: (0, 0, 0, 0)),
            pl.BlockSpec((n_track, EPOCHS, 128), lambda g: (0, 0, 0)),
            pl.BlockSpec((n_knots, EPOCHS), lambda g: (0, 0)),
            pl.BlockSpec((n_track, 3, block), lambda g: (0, 0, g)),
        ],
        out_specs=(
            pl.BlockSpec((3, EPOCHS, block), lambda g: (0, 0, g)),
            pl.BlockSpec((3, n_knots, block), lambda g: (0, 0, g)),
        ),
        compiler_params=pltpu.CompilerParams(vmem_limit_bytes=60 << 20),
        name="geometry",
    )(gathered, r, meta, fitter, look_local))


def solution(mesh):
    sizes = tuple(mesh.shape[name] for name in ("track", "ifg", "pix"))
    in_specs = (P("track", "ifg", "pix"), P("track", "ifg", None), P(), P(), P(None, None, "pix"))
    out_specs = (P(None, None, ("pix", "ifg", "track")), P(None, None, ("pix", "ifg", "track")))
    return jax.shard_map(functools.partial(shards, sizes), mesh=mesh, in_specs=in_specs, out_specs=out_specs, check_vma=False)
```
